32 devices in a mesh: blk: 8 (over z, y), grp: 4 (over x, core).
Axes of the slice: x: 2, y: 2, z: 4, core: 2. Of those that a mesh axis runs over, the one named last changes fastest.
Arguments:
- start_state: float32 [64, 4096], P(('blk', 'grp')), may hold values from -6 to 6
- start_log_weight: float32 [64], P(('blk', 'grp')), may hold values from -10 to 330
- noise: bfloat16 [3, 64, 4096], P(None, ('blk', 'grp')), may hold values from -6 to 6
- first_weight: bfloat16 [14336, 4096], P('blk'), may hold values from -0.09375 to 0.09375
- second_weight: bfloat16 [14336, 4096], P('blk'), may hold values from -0.09375 to 0.09375
- third_weight: bfloat16 [14336, 4096], P('blk'), may hold values from -0.09375 to 0.09375
Outputs:
- final_state: float32 [64, 4096], P(('blk', 'grp'))
- log_weight: float32 [64], P(('blk', 'grp'))
- log_ratio: float32 [], replicated
The draws below stay inside these ranges and needn't reach their ends.
All inputs are finite; a program needn't handle non-finite values.
Results may differ from the reference program's by a relative error of at most 0.00074.
Values may be sent and summed in bfloat16 or wider, within the bound.
No kernel may reach another device: no remote copies, remote signals or barrier semaphores. Data moves between devices by JAX's collectives and lax.ppermute only.
A program may use at most 128 MiB of HBM per device.

```python
import math
import jax
import jax.numpy as jnp
from jax import lax

D = 4096
FF = 14336
STEPS = 3
CHAINS = 64


def draw_start_log_weight(key, part):
    base_key = jax.random.fold_in(key, 11)
    level_key = jax.random.fold_in(key, 12)
    order_key = jax.random.fold_in(key, 13)
    spread_key = jax.random.fold_in(key, 14)
    values = 2.0 * jax.random.normal(base_key, (CHAINS,), jnp.float32)
    values = jnp.clip(values, -8.0, 8.0)
    level = jax.random.uniform(level_key, (), jnp.float32, 105.0, 140.0)
    chosen = jax.random.permutation(order_key, CHAINS)[:3]
    offsets = jnp.array([0.0, 1.5, 2.7], jnp.float32) + jax.random.uniform(spread_key, (3,), jnp.float32, 0.0, 0.2)
    values = values.at[chosen].set(level - offsets)
    return values.astype(jnp.float32)


def block_levels(rng, extent, pieces, least, largest):
    def one(dim, shards_of):
        draws = jax.random.uniform(jax.random.fold_in(jax.random.fold_in(rng, 6), dim), (shards_of,), jnp.float32, least / len(pieces), largest / len(pieces))
        return jnp.repeat(jnp.exp(draws), extent[dim] // shards_of).reshape((-1,) + (1,) * (len(extent) - dim - 1))

    gain = one(*pieces[0])
    for cut in pieces[1:]:
        gain = gain * one(*cut)
    return gain


def bell_draw(stream_key, shape, scale, limit, pieces=(), dtype=jnp.bfloat16):
    gain = block_levels(stream_key, shape, pieces, -0.22, 0.18) if pieces else 1.0
    values = jax.random.normal(stream_key, shape, jnp.float32) * scale * gain
    return jnp.minimum(jnp.maximum(values, -limit), limit).astype(dtype)


def setup_inputs(seed: int = 0) -> dict:
    arg_keys = jax.random.split(jax.random.key(seed), 7)
    return {
        "start_state": bell_draw(arg_keys[0], (CHAINS, D), 1.0, 6.0, ((0, 32),), jnp.float32),
        "start_log_weight": draw_start_log_weight(jax.random.fold_in(arg_keys[6], 71), 0),
        "noise": bell_draw(arg_keys[2], (STEPS, CHAINS, D), 1.0, 6.0, ((1, 32),)),
        "first_weight": bell_draw(arg_keys[3], (FF, D), D ** -0.5, 0.09375, ((0, 8),)),
        "second_weight": bell_draw(arg_keys[4], (FF, D), D ** -0.5, 0.09375, ((0, 8),)),
        "third_weight": bell_draw(arg_keys[5], (FF, D), D ** -0.5, 0.09375, ((0, 8),)),
    }


def reference(start_state, start_log_weight, noise, first_weight, second_weight, third_weight):
    state = start_state
    log_weight = start_log_weight
    dims = (((1,), (1,)), ((), ()))
    for step in range(STEPS):
        rounded = state.astype(jnp.bfloat16)
        pre_a = lax.dot_general(rounded, first_weight, dims, preferred_element_type=jnp.float32)
        pre_b = lax.dot_general(rounded, second_weight, dims, preferred_element_type=jnp.float32)
        pre_c = lax.dot_general(rounded, third_weight, dims, preferred_element_type=jnp.float32)
        soft = jax.nn.softplus(pre_a)
        tan_b = jnp.tanh(pre_b)
        energy = lax.optimization_barrier(jnp.sum(soft * tan_b * pre_c, axis=1))
        factor_a = (jax.nn.sigmoid(pre_a) * tan_b * pre_c).astype(jnp.bfloat16)
        factor_b = (soft * (1.0 - tan_b * tan_b) * pre_c).astype(jnp.bfloat16)
        factor_c = (soft * tan_b).astype(jnp.bfloat16)
        gradient = jnp.dot(factor_a, first_weight, preferred_element_type=jnp.float32)
        gradient = gradient + jnp.dot(factor_b, second_weight, preferred_element_type=jnp.float32)
        gradient = gradient + jnp.dot(factor_c, third_weight, preferred_element_type=jnp.float32)
        log_weight = log_weight - energy / STEPS
        beta = (step + 1) / STEPS
        state = state - 0.05 * (state + beta * gradient) + math.sqrt(0.1) * noise[step].astype(jnp.float32)
    top = jnp.max(log_weight)
    total = jnp.sum(jnp.exp(log_weight - top))
    log_ratio = top + jnp.log(total) - math.log(CHAINS)
    return (state, log_weight, log_ratio)
```

```python
import functools
import math

import jax
import jax.numpy as jnp
from jax import lax
from jax.experimental import pallas as pl
from jax.experimental.pallas import tpu as pltpu
from jax.sharding import Mesh
from jax.sharding import PartitionSpec as P

LANES = 128


def chunk_rows(rows):
    return 128 if rows % 128 == 0 else rows


def column_tile(columns):
    return 512 if columns % 512 == 0 else columns


def lane_width(count):
    return -(-count // LANES) * LANES


def as_row(column, width):
    spread = jnp.broadcast_to(column, (column.shape[0], LANES))
    spread = jnp.pad(spread, ((0, width - column.shape[0]), (0, 0)))
    return spread.T[:1, :]


def paired(first, second, rows):
    shape = (rows, first.shape[1])
    odd = lax.broadcasted_iota(jnp.int32, shape, 0) % 2 == 1
    return jnp.where(odd, jnp.broadcast_to(second, shape), jnp.broadcast_to(first, shape))


def step_kernel(
    mine_ref, other_ref, base_ref, w1_ref, w2_ref, w3_ref,
    mine_out, other_out, next_base, held, factors, sems, *, last, steps,
):
    hidden, columns = held.shape[1], held.shape[2]
    near = mine_ref.shape[0]
    chunk = chunk_rows(hidden)
    start = lax.axis_index("half") * hidden
    sources = (w1_ref, w2_ref, w3_ref)
    copies = []
    for j in range(hidden // chunk):
        for i in range(3):
            copy = pltpu.make_async_copy(
                sources[i].at[pl.ds(pl.multiple_of(start + j * chunk, 16), chunk)],
                held.at[i, pl.ds(j * chunk, chunk)],
                sems.at[j, i],
            )
            copy.start()
            copies.append(copy)
    state = jnp.concatenate([mine_ref[...], other_ref[...]], axis=0)
    contract = (((1,), (1,)), ((), ()))
    energy = jnp.zeros((state.shape[0], 1), jnp.float32)
    for j in range(hidden // chunk):
        rows = pl.ds(j * chunk, chunk)
        pre = []
        for i in range(3):
            copies[3 * j + i].wait()
        for i in range(3):
            pre.append(
                lax.dot_general(state, held[i, rows], contract, preferred_element_type=jnp.float32)
            )
        pre_a, pre_b, pre_c = pre
        decay = jnp.exp(-jnp.abs(pre_a))
        soft = jnp.maximum(pre_a, 0.0) + jnp.log1p(decay)
        sigma = jnp.where(pre_a >= 0.0, 1.0, decay) / (1.0 + decay)
        tan_b = jnp.tanh(pre_b)
        soft_tan = soft * tan_b
        energy = energy + jnp.sum(soft_tan * pre_c, axis=1, keepdims=True)
        factors[0, :, rows] = (sigma * tan_b * pre_c).astype(jnp.bfloat16)
        factors[1, :, rows] = (soft * (1.0 - tan_b * tan_b) * pre_c).astype(jnp.bfloat16)
        factors[2, :, rows] = soft_tan.astype(jnp.bfloat16)
    width = base_ref.shape[1]
    shift = energy / steps
    mine_row = base_ref[0:1, :] - as_row(shift[:near], width)
    other_row = base_ref[1:2, :] - as_row(shift[near:], width)
    if last:
        mine_out[:, columns:] = paired(mine_row, other_row, near)
        other_out[:, columns:] = paired(other_row, mine_row, near)
    next_base[...] = paired(mine_row, other_row, 8)
    tile = column_tile(columns)
    for j in range(columns // tile):
        cols = pl.ds(j * tile, tile)
        total = jnp.dot(factors[0], held[0, :, cols], preferred_element_type=jnp.float32)
        total = total + jnp.dot(factors[1], held[1, :, cols], preferred_element_type=jnp.float32)
        total = total + jnp.dot(factors[2], held[2, :, cols], preferred_element_type=jnp.float32)
        mine_out[:, cols] = total[:near]
        other_out[:, cols] = total[near:]


def head_step(mine, other, base, weights, hidden, last, steps):
    near, columns = mine.shape
    width = base.shape[1]
    chunk = chunk_rows(hidden)
    wide = columns + width if last else columns
    vmem = pl.BlockSpec(memory_space=pltpu.VMEM)
    return pl.pallas_call(
        functools.partial(step_kernel, last=last, steps=steps),
        out_shape=(
            jax.ShapeDtypeStruct((near, wide), jnp.float32),
            jax.ShapeDtypeStruct((near, wide), jnp.float32),
            jax.ShapeDtypeStruct((8, width), jnp.float32),
        ),
        in_specs=[vmem] * 3 + [pl.BlockSpec(memory_space=pl.ANY)] * 3,
        out_specs=(vmem,) * 3,
        scratch_shapes=[
            pltpu.VMEM((3, hidden, columns), jnp.bfloat16),
            pltpu.VMEM((3, 2 * near, hidden), jnp.bfloat16),
            pltpu.SemaphoreType.DMA((hidden // chunk, 3)),
        ],
        compiler_params=pltpu.CompilerParams(vmem_limit_bytes=40 * 1024 * 1024),
        cost_estimate=pl.CostEstimate(
            flops=24 * near * hidden * columns,
            bytes_accessed=6 * hidden * columns,
            transcendentals=8 * near * hidden,
        ),
        name="head_step",
    )(mine, other, base, *weights)


def per_device(start_state, start_log_weight, noise, first_weight, second_weight, third_weight):
    steps = noise.shape[0]
    own, columns = start_state.shape
    weights = (first_weight, second_weight, third_weight)
    peers, halves, planes = lax.axis_size("blk"), lax.axis_size("half"), lax.axis_size("side")
    assert halves == 2
    hidden = first_weight.shape[0] // halves
    near = peers * own
    width = lane_width(near)
    at = lax.axis_index("blk") * own

    def exchange(value):
        return lax.all_to_all(value, "blk", 0, 0, tiled=True)

    def swap(value):
        return lax.ppermute(value, "half", [(0, 1), (1, 0)])

    base = lax.dynamic_update_slice(jnp.zeros((8, width), jnp.float32), start_log_weight[None], (0, at))
    state = start_state
    for step in range(steps):
        last = step == steps - 1
        rounded = state.astype(jnp.bfloat16)
        mine = exchange(jnp.broadcast_to(rounded[None], (peers, own, columns))).reshape(near, columns)
        other = swap(mine)
        mine_part, other_part, base = head_step(mine, other, base, weights, hidden, last, steps)
        part = mine_part + swap(other_part)
        got = jnp.sum(exchange(part.reshape(peers, own, part.shape[1])), axis=0)
        gradient = got[:, :columns]
        beta = (step + 1) / steps
        state = (
            state
            - 0.05 * (state + beta * gradient)
            + math.sqrt(0.1) * noise[step].astype(jnp.float32)
        )
    plane = got[:, columns : columns + near]
    log_weight = lax.dynamic_slice_in_dim(plane[0], at, own, 0)
    top = jnp.max(plane)
    total = jnp.sum(jnp.exp(plane - top))
    pair = jnp.stack([top, total])
    pairs = [pair]
    for shift in range(1, planes):
        pairs.append(lax.ppermute(pair, "side", [(a, (a + shift) % planes) for a in range(planes)]))
    tops = jnp.stack([p[0] for p in pairs])
    totals = jnp.stack([p[1] for p in pairs])
    top = jnp.max(tops)
    total = jnp.sum(totals * jnp.exp(tops - top))
    log_ratio = top + jnp.log(total) - math.log(near * halves * planes)
    return (state, log_weight, log_ratio)


def solution(mesh):
    blk, grp = mesh.shape["blk"], mesh.shape["grp"]
    fine = Mesh(mesh.devices.reshape(blk, grp // 2, 2), ("blk", "side", "half"))
    every = ("blk", "side", "half")
    placed = (
        P(every, None),
        P(every),
        P(None, every, None),
        P("blk", None),
        P("blk", None),
        P("blk", None),
    )
    return jax.shard_map(
        per_device,
        mesh=fine,
        in_specs=placed,
        out_specs=(P(every, None), P(every), P()),
        check_vma=False,
    )
```

```python
import functools
import math

import jax
import jax.numpy as jnp
from jax import lax
from jax.experimental import pallas as pl
from jax.experimental.pallas import tpu as pltpu
from jax.sharding import Mesh
from jax.sharding import PartitionSpec as P

LANES = 128
GRANT = 16 * 1024 * 1024


def chunk_rows(rows):
    return 128 if rows % 128 == 0 else rows


def column_tile(columns):
    return 512 if columns % 512 == 0 else columns


def lane_width(count):
    return -(-count // LANES) * LANES


def stack_rows(mine_ref, other_ref, rows_ref):
    peers, own = mine_ref.shape[0], mine_ref.shape[1]
    for k, ref in enumerate((mine_ref, other_ref)):
        for d in range(peers):
            rows_ref[pl.ds((k * peers + d) * own, own), :] = ref[d].astype(jnp.float32)
    return rows_ref[...].astype(jnp.bfloat16)


def put_rows(out, cols, rows):
    own = out.shape[1]
    for d in range(out.shape[0]):
        out[d, :, cols] = rows[d * own : (d + 1) * own]


def as_row(column, width):
    spread = jnp.broadcast_to(column, (column.shape[0], LANES))
    spread = jnp.pad(spread, ((0, width - column.shape[0]), (0, 0)))
    return spread.T[:1, :]


def paired(first, second, rows):
    shape = (rows, first.shape[1])
    odd = lax.broadcasted_iota(jnp.int32, shape, 0) % 2 == 1
    return jnp.where(odd, jnp.broadcast_to(second, shape), jnp.broadcast_to(first, shape))


def factors_of(pre_a, pre_b, pre_c):
    decay = jnp.exp(-jnp.abs(pre_a))
    soft = jnp.maximum(pre_a, 0.0) + jnp.log1p(decay)
    sigma = jnp.where(pre_a >= 0.0, 1.0, decay) / (1.0 + decay)
    tan_b = jnp.tanh(pre_b)
    soft_tan = soft * tan_b
    return (
        jnp.sum(soft_tan * pre_c, axis=1, keepdims=True),
        (sigma * tan_b * pre_c).astype(jnp.bfloat16),
        (soft * (1.0 - tan_b * tan_b) * pre_c).astype(jnp.bfloat16),
        soft_tan.astype(jnp.bfloat16),
    )


def project(state, held, i, rows):
    contract = (((1,), (1,)), ((), ()))
    return lax.dot_general(state, held[i, rows], contract, preferred_element_type=jnp.float32)


def finish(energy, base_ref, mine_out, other_out, next_base, held, factors, last, steps):
    near, columns = mine_out.shape[0] * mine_out.shape[1], held.shape[2]
    width = base_ref.shape[1]
    shift = energy / steps
    mine_row = base_ref[0:1, :] - as_row(shift[:near], width)
    other_row = base_ref[1:2, :] - as_row(shift[near:], width)
    if last:
        tail = pl.ds(columns, width)
        put_rows(mine_out, tail, paired(mine_row, other_row, near))
        put_rows(other_out, tail, paired(other_row, mine_row, near))
    next_base[...] = paired(mine_row, other_row, 8)
    tile = column_tile(columns)
    for j in range(columns // tile):
        cols = pl.ds(j * tile, tile)
        total = jnp.dot(factors[0], held[0, :, cols], preferred_element_type=jnp.float32)
        total = total + jnp.dot(factors[1], held[1, :, cols], preferred_element_type=jnp.float32)
        total = total + jnp.dot(factors[2], held[2, :, cols], preferred_element_type=jnp.float32)
        put_rows(mine_out, cols, total[:near])
        put_rows(other_out, cols, total[near:])


def first_kernel(
    mine_ref, other_ref, base_ref, w1_ref, w2_ref, w3_ref,
    mine_out, other_out, next_base, held, rows_ref, factors, sems, *, last, steps,
):
    hidden = held.shape[1]
    chunk = chunk_rows(hidden)
    start = lax.axis_index("half") * hidden
    sources = (w1_ref, w2_ref, w3_ref)
    copies = []
    for j in range(hidden // chunk):
        for i in range(3):
            copy = pltpu.make_async_copy(
                sources[i].at[pl.ds(pl.multiple_of(start + j * chunk, 16), chunk)],
                held.at[i, pl.ds(j * chunk, chunk)],
                sems.at[j, i],
            )
            copy.start()
            copies.append(copy)
    state = stack_rows(mine_ref, other_ref, rows_ref)
    energy = jnp.zeros((state.shape[0], 1), jnp.float32)
    for j in range(hidden // chunk):
        rows = pl.ds(j * chunk, chunk)
        for i in range(3):
            copies[3 * j + i].wait()
        share, *found = factors_of(*(project(state, held, i, rows) for i in range(3)))
        energy = energy + share
        for i in range(3):
            factors[i, :, rows] = found[i]
    finish(energy, base_ref, mine_out, other_out, next_base, held, factors, last, steps)


def later_kernel(
    mine_ref, other_ref, base_ref, held, mine_out, other_out, next_base, rows_ref, factors,
    *, last, steps,
):
    state = stack_rows(mine_ref, other_ref, rows_ref)
    every = pl.ds(0, held.shape[1])
    energy, *found = factors_of(*(project(state, held, i, every) for i in range(3)))
    for i in range(3):
        factors[i] = found[i]
    finish(energy, base_ref, mine_out, other_out, next_base, held, factors, last, steps)


def head_step(mine, other, base, weights, held, hidden, last, steps):
    peers, own, columns = mine.shape
    near = peers * own
    width = base.shape[1]
    chunk = chunk_rows(hidden)
    wide = columns + width if last else columns
    vmem = pl.BlockSpec(memory_space=pltpu.VMEM)
    results = [
        jax.ShapeDtypeStruct((peers, own, wide), jnp.float32),
        jax.ShapeDtypeStruct((peers, own, wide), jnp.float32),
        jax.ShapeDtypeStruct((8, width), jnp.float32),
    ]
    scratch = [
        pltpu.VMEM((2 * near, columns), jnp.float32),
        pltpu.VMEM((3, 2 * near, hidden), jnp.bfloat16),
    ]
    if held is None:
        kernel = first_kernel
        sources = tuple(pltpu.with_memory_space_constraint(w, pltpu.HBM) for w in weights)
        specs = [pl.BlockSpec(memory_space=pltpu.HBM)] * 3
        results.append(pltpu.VMEM((3, hidden, columns), jnp.bfloat16))
        scratch.append(pltpu.SemaphoreType.DMA((hidden // chunk, 3)))
    else:
        kernel, specs = later_kernel, [vmem]
        sources = (pltpu.with_memory_space_constraint(held, pltpu.VMEM),)
    return pl.pallas_call(
        functools.partial(kernel, last=last, steps=steps),
        out_shape=tuple(results),
        in_specs=[vmem] * 3 + specs,
        out_specs=(vmem,) * len(results),
        scratch_shapes=scratch,
        compiler_params=pltpu.CompilerParams(vmem_limit_bytes=GRANT),
        cost_estimate=pl.CostEstimate(
            flops=24 * near * hidden * columns,
            bytes_accessed=6 * hidden * columns,
            transcendentals=8 * near * hidden,
        ),
        name="head_step",
    )(mine, other, base, *sources)


def update_kernel(got_ref, state_ref, noise_ref, state_out, second_out, *, step, steps):
    own, columns = state_ref.shape
    got = got_ref[0]
    for d in range(1, got_ref.shape[0]):
        got = got + got_ref[d]
    beta = (step + 1) / steps
    state = state_ref[...]
    state = (
        state
        - 0.05 * (state + beta * got[:, :columns])
        + math.sqrt(0.1) * noise_ref[step].astype(jnp.float32)
    )
    state_out[...] = state
    if step < steps - 1:
        rounded = state.astype(jnp.bfloat16)
        for d in range(second_out.shape[0]):
            second_out[d] = rounded
        return
    near = got_ref.shape[0] * own
    width = got.shape[1] - columns
    plane = got[:, columns:]
    inside = lax.broadcasted_iota(jnp.int32, plane.shape, 1) < near
    valid = jnp.where(inside, plane, -jnp.inf)
    top = jnp.max(jnp.max(valid, axis=1, keepdims=True), axis=0, keepdims=True)
    shares = jnp.sum(jnp.exp(valid - top), axis=1, keepdims=True)
    total = jnp.sum(shares, axis=0, keepdims=True)
    shape = second_out.shape
    row = lax.broadcasted_iota(jnp.int32, shape, 0)
    at = lax.axis_index("blk") * own
    mine = pltpu.roll(jnp.broadcast_to(plane[0:1, :], shape), (width - at) % width, 1)
    second_out[...] = jnp.where(row == 0, top, jnp.where(row == 1, total, mine))


def update(got, state, noise, step):
    steps = noise.shape[0]
    vmem = pl.BlockSpec(memory_space=pltpu.VMEM)
    if step < steps - 1:
        second = jax.ShapeDtypeStruct((got.shape[0],) + state.shape, jnp.bfloat16)
    else:
        second = jax.ShapeDtypeStruct((8, got.shape[2] - state.shape[1]), jnp.float32)
    return pl.pallas_call(
        functools.partial(update_kernel, step=step, steps=steps),
        out_shape=(jax.ShapeDtypeStruct(state.shape, jnp.float32), second),
        in_specs=[vmem] * 3,
        out_specs=(vmem, vmem),
        compiler_params=pltpu.CompilerParams(vmem_limit_bytes=GRANT),
        name="update",
    )(got, state, noise)


def merge_kernel(*refs, chains):
    out_ref = refs[-1]
    top = refs[0][0:1, :LANES]
    for ref in refs[1:-1]:
        top = jnp.maximum(top, ref[0:1, :LANES])
    total = jnp.zeros_like(top)
    for ref in refs[:-1]:
        total = total + ref[1:2, :LANES] * jnp.exp(ref[0:1, :LANES] - top)
    out_ref[...] = top + jnp.log(total) - math.log(chains)


def merge(blocks, chains):
    vmem = pl.BlockSpec(memory_space=pltpu.VMEM)
    return pl.pallas_call(
        functools.partial(merge_kernel, chains=chains),
        out_shape=jax.ShapeDtypeStruct((1, LANES), jnp.float32),
        in_specs=[vmem] * len(blocks),
        out_specs=vmem,
        compiler_params=pltpu.CompilerParams(vmem_limit_bytes=1 << 20),
        name="merge",
    )(*blocks)


def per_device(start_state, start_log_weight, noise, first_weight, second_weight, third_weight):
    steps = noise.shape[0]
    own, columns = start_state.shape
    weights = (first_weight, second_weight, third_weight)
    peers, halves, planes = lax.axis_size("blk"), lax.axis_size("half"), lax.axis_size("side")
    assert halves == 2
    hidden = first_weight.shape[0] // halves
    near = peers * own
    width = lane_width(near)
    at = lax.axis_index("blk") * own

    def exchange(value):
        return lax.all_to_all(value, "blk", 0, 0, tiled=True)

    def swap(value):
        return lax.ppermute(value, "half", [(0, 1), (1, 0)])

    base = lax.dynamic_update_slice(jnp.zeros((8, width), jnp.float32), start_log_weight[None], (0, at))
    state, held = start_state, None
    copies = jnp.broadcast_to(state.astype(jnp.bfloat16)[None], (peers, own, columns))
    for step in range(steps):
        last = step == steps - 1
        mine = exchange(copies)
        other = swap(mine)
        mine_part, other_part, base, *kept = head_step(mine, other, base, weights, held, hidden, last, steps)
        held = kept[0] if kept else held
        state, copies = update(exchange(mine_part + swap(other_part)), state, noise, step)
    block = copies
    blocks = [block]
    for shift in range(1, planes):
        blocks.append(lax.ppermute(block, "side", [(a, (a + shift) % planes) for a in range(planes)]))
    log_weight = block[2, :own]
    log_ratio = merge(blocks, near * halves * planes)[0, 0]
    return (state, log_weight, log_ratio)


def solution(mesh):
    blk, grp = mesh.shape["blk"], mesh.shape["grp"]
    fine = Mesh(mesh.devices.reshape(blk, grp // 2, 2), ("blk", "side", "half"))
    every = ("blk", "side", "half")
    placed = (
        P(every, None),
        P(every),
        P(None, every, None),
        P("blk", None),
        P("blk", None),
        P("blk", None),
    )
    return jax.shard_map(
        per_device,
        mesh=fine,
        in_specs=placed,
        out_specs=(P(every, None), P(every), P()),
        check_vma=False,
    )
```
